32 devices in a mesh: pool: 16 (over z, y, x), serve: 2 (over core).
Axes of the slice: x: 2, y: 2, z: 4, core: 2. Of those that a mesh axis runs over, the one named last changes fastest.
Arguments:
- queries: bfloat16 [2, 256, 73728], P('serve', None, 'pool'), may hold values from -16 to 16
- new_latent: bfloat16 [2, 147456], P('serve', 'pool'), may hold values from -8 to 8
- pool: bfloat16 [2, 192, 36864], P('serve', 'pool'), may hold values from -6 to 6
- page_owner: int32 [2, 32], P('serve'), may hold values from 0 to 15, as said below
- page_slot: int32 [2, 32], P('serve'), may hold values from 0 to 10
- new_owner: int32 [2, 4], P('serve'), may hold values from 0 to 15, as said below
- new_slot: int32 [2, 4], P('serve'), may hold values from 0 to 11
- prefix_len: int32 [2], P('serve'), may hold values from 512 to 2048, as said below
- w_uv: bfloat16 [128, 512, 128], P('pool', 'serve'), may hold values from -1 to 1
Outputs:
- attn_out: bfloat16 [2, 256, 16384], P('serve', None, 'pool')
- new_pool: bfloat16 [2, 192, 36864], P('serve', 'pool')
The draws below stay inside these ranges and needn't reach their ends.
Inputs may be any that keep to these rules, and one draw needn't show every extreme that they name: Within a request the pairs (page_owner, page_slot) differ from one another and from the pairs (new_owner, new_slot); at most 3 entries of a request's table name the same owner, and in every request some owner is named exactly 3 times. `new_owner`: the 4 new pages of a request go to different owners. `prefix_len`: some request has exactly 2048 prefix tokens.
All inputs are finite; a program needn't handle non-finite values.
Results may differ from the reference program's by a relative error of at most 0.0075.
Values may be sent and summed in bfloat16 or wider, within the bound.
A program may use at most 128 MiB of HBM per device.

```python
import jax
import jax.numpy as jnp
from jax import lax

HEADS = 128
VLAT = 512
VHEAD = 128
PAGE = 64
SUF = 256
PMAX = 2048
HOT = 3
LAT = 576
PPAGES = 32
NEWP = 4
SLOTS = 12
REQS = 2
N_POOL = 16


def drawn_pair(key):
    folded = jax.random.fold_in(key, 17)
    latent_key, query_key = jax.random.split(folded, 2)
    latent = jax.random.truncated_normal(latent_key, -6.0, 6.0, (REQS, SUF, LAT), jnp.float32)
    queries = jax.random.truncated_normal(query_key, -6.0, 6.0, (REQS, SUF, HEADS, LAT), jnp.float32)
    return (queries.reshape(REQS, SUF, HEADS * LAT), latent.reshape(REQS, SUF * LAT))


def page_tables(key):
    folded = jax.random.fold_in(key, 29)

    def per_request(request_key):
        hot_key, score_key, shuffle_key, slot_key, fresh_key = jax.random.split(request_key, 5)
        owner_key, order_key = jax.random.split(fresh_key)
        tickets = jnp.arange(N_POOL * HOT, dtype=jnp.int32)
        ticket_owner = tickets // HOT
        ticket_rank = tickets % HOT
        hottest = jax.random.randint(hot_key, (), 0, N_POOL, dtype=jnp.int32)
        ticket_score = jax.random.randint(score_key, (N_POOL * HOT,), 0, 1 << 16, dtype=jnp.int32) * (N_POOL * HOT) + tickets
        ticket_score = jnp.where(ticket_owner == hottest, tickets - N_POOL * HOT, ticket_score)
        ordering = jnp.argsort(ticket_score, stable=True)[:PPAGES].astype(jnp.int32)
        ordering = ordering[jax.random.permutation(shuffle_key, PPAGES)]
        page_owners = ticket_owner[ordering]
        page_ranks = ticket_rank[ordering]
        slot_scores = jax.random.randint(slot_key, (N_POOL, SLOTS - 1), 0, 1 << 16, dtype=jnp.int32) * SLOTS + jnp.arange(SLOTS - 1, dtype=jnp.int32)[None, :]
        small_order = jnp.argsort(slot_scores, axis=1, stable=True).astype(jnp.int32)
        last_column = jnp.full((N_POOL, 1), SLOTS - 1, jnp.int32)
        slot_order = jnp.concatenate([small_order[:, :HOT], last_column, small_order[:, HOT:]], 1).astype(jnp.int32)
        page_slots = slot_order[page_owners, page_ranks]
        others = jax.random.permutation(owner_key, N_POOL - 1)[:NEWP - 1].astype(jnp.int32)
        fresh_owners = jnp.concatenate([others, jnp.full((1,), N_POOL - 1, jnp.int32)], 0)
        fresh_owners = fresh_owners[jax.random.permutation(order_key, NEWP)].astype(jnp.int32)
        fresh_slots = slot_order[fresh_owners, HOT + jnp.arange(NEWP, dtype=jnp.int32)]
        return (page_owners, page_slots, fresh_owners, fresh_slots)
    return jax.vmap(per_request)(jax.random.split(folded, REQS))


def draw_queries(key, part):
    return drawn_pair(key)[0].astype(jnp.bfloat16)


def draw_new_latent(key, part):
    return drawn_pair(key)[1].astype(jnp.bfloat16)


def draw_page_owner(key, part):
    return page_tables(key)[0].astype(jnp.int32)


def draw_page_slot(key, part):
    return page_tables(key)[1].astype(jnp.int32)


def draw_new_owner(key, part):
    return page_tables(key)[2].astype(jnp.int32)


def draw_new_slot(key, part):
    return page_tables(key)[3].astype(jnp.int32)


def draw_prefix_len(key, part):
    length_key, top_key = jax.random.split(jax.random.fold_in(key, 41))
    lengths = jax.random.randint(length_key, (REQS,), PMAX // 4, PMAX + 1, dtype=jnp.int32)
    longest = jax.random.randint(top_key, (), 0, REQS, dtype=jnp.int32)
    return jnp.where(jnp.arange(REQS, dtype=jnp.int32) == longest, PMAX, lengths).astype(jnp.int32)


def level_of(own_key, dims, cuts, low, top_value):
    level, own = 1.0, jax.random.fold_in(own_key, 6)
    for dim, blocks in cuts:
        draws = jnp.exp(jax.random.uniform(jax.random.fold_in(own, dim), (blocks,), jnp.float32, low / len(cuts), top_value / len(cuts)))
        level = level * jnp.repeat(draws, dims[dim] // blocks).reshape([-1 if axis == dim else 1 for axis in range(len(dims))])
    return level


def bell_draw(stream_key, extent, spread, limit, pieces=(), kind=jnp.bfloat16):
    loudness = level_of(stream_key, extent, pieces, -0.22, 0.18) if pieces else 1.0
    result = jax.random.normal(stream_key, extent, jnp.float32) * spread * loudness
    return jnp.minimum(jnp.maximum(result, -limit), limit).astype(kind)


def setup_inputs(seed: int = 0) -> dict:
    seeds = jax.random.split(jax.random.key(seed), 10)
    return {
        "queries": draw_queries(jax.random.fold_in(seeds[9], 71), 0),
        "new_latent": draw_new_latent(jax.random.fold_in(seeds[9], 71), 0),
        "pool": bell_draw(seeds[2], (REQS, N_POOL * SLOTS, PAGE * LAT), 1.0, 6.0, ((0, 2), (1, 16))),
        "page_owner": draw_page_owner(jax.random.fold_in(seeds[9], 71), 0),
        "page_slot": draw_page_slot(jax.random.fold_in(seeds[9], 71), 0),
        "new_owner": draw_new_owner(jax.random.fold_in(seeds[9], 71), 0),
        "new_slot": draw_new_slot(jax.random.fold_in(seeds[9], 71), 0),
        "prefix_len": draw_prefix_len(jax.random.fold_in(seeds[9], 71), 0),
        "w_uv": bell_draw(seeds[8], (HEADS, VLAT, VHEAD), (VLAT // 16) ** -0.5, 1.0, ((0, 16), (1, 2))),
    }


softmax_scale = 192.0 ** -0.5
masked_score = -1e30


def reference(queries, new_latent, pool, page_owner, page_slot, new_owner, new_slot, prefix_len, w_uv):
    def per_request(operands):
        query_rows, latent_rows, pool_pages, owners, slot_ids, fresh_owners, fresh_slots, length = operands
        page_rows = (owners * SLOTS + slot_ids).astype(jnp.int32)
        prefix = pool_pages[page_rows].reshape(PPAGES * PAGE, LAT)
        suffix = latent_rows.reshape(SUF, LAT)
        key_rows = jnp.concatenate([prefix, suffix], 0)
        value_rows = key_rows[:, :VLAT]
        position = jnp.arange(PPAGES * PAGE, dtype=jnp.int32)
        earlier = jnp.broadcast_to(position[None, :] < length, (SUF, PPAGES * PAGE))
        query_pos = jnp.arange(SUF, dtype=jnp.int32)
        causal = query_pos[None, :] <= query_pos[:, None]
        allowed = jnp.concatenate([earlier, causal], 1)
        head_queries = query_rows.reshape(SUF, HEADS, LAT).transpose(1, 0, 2)

        def per_head(head_operands):
            one_head, head_weight = head_operands
            scores = jnp.dot(one_head, key_rows.T, preferred_element_type=jnp.float32) * softmax_scale
            scores = jnp.where(allowed, scores, masked_score)
            top_score = jnp.max(scores, axis=1, keepdims=True)
            weights = jnp.exp(scores - top_score)
            weight_sum = jnp.sum(weights, axis=1, keepdims=True)
            mixture = jnp.dot(weights.astype(jnp.bfloat16), value_rows, preferred_element_type=jnp.float32) / weight_sum
            return jnp.dot(mixture.astype(jnp.bfloat16), head_weight, preferred_element_type=jnp.float32).astype(jnp.bfloat16)

        outputs = lax.map(per_head, (head_queries, w_uv))
        attended = outputs.transpose(1, 0, 2).reshape(SUF, HEADS * VHEAD)
        targets = (fresh_owners * SLOTS + fresh_slots).astype(jnp.int32)
        updated = pool_pages.at[targets].set(latent_rows.reshape(NEWP, PAGE * LAT))
        return attended, updated

    attn_out, new_pool = lax.map(per_request, (queries, new_latent, pool, page_owner, page_slot, new_owner, new_slot, prefix_len))
    return attn_out, new_pool
```

```python
import functools

import jax
import jax.numpy as jnp
from jax import lax
from jax.experimental import pallas as pl
from jax.experimental.pallas import tpu as pltpu
from jax.sharding import PartitionSpec as P

VLAT = 512
VHEAD = 128
PAGE = 64
SUF = 256
HOT = 3
LAT = 576
PPAGES = 32
NEWP = 4
SLOTS = 12

LANES = 128
ROPE = LAT - VLAT
WIDE = VLAT + LANES
PAIR = PAGE // 2
PAIR_ROWS = 2 * LAT // LANES
FLAT = PAGE * LAT // LANES
BLOCK = HOT * PAGE
SHELF = 16
TILE = 512
SUB = 256

softmax_scale = 192.0 ** (-0.5)
masked_score = -1e30
exp2_scale = softmax_scale * 1.4426950408889634

MESH = pl.DeviceIdType.MESH
contract_last = (((1,), (1,)), ((), ()))


def fused_kernel(n, serve_n, table_ref, owners_ref, raw_ref, pool_hbm, q_hbm, w_hbm, out_ref, new_ref,
                 pool_ref, poolf_ref, flat_ref, q_ref, w_ref, wg_ref, qs_ref, lat_ref, rope_ref,
                 kr_ref, raws_ref, rawf_ref, sfx_ref, count_ref, s_ref, acc_ref, top_ref, sum_ref,
                 local_sem, z_send, z_recv, x_send, x_recv, y_send, y_recv, w_send, w_recv,
                 r_send, r_recv):
    depth = n // 4
    heads = q_ref.shape[1] // LAT
    raw_rows = raw_ref.shape[0]
    me = lax.axis_index("pool")
    core = lax.axis_index("serve")
    x = me % 2
    y = (me // 2) % 2
    z = me // 4
    x_peer = z * 4 + y * 2 + (1 - x)
    y_peer = z * 4 + (1 - y) * 2 + x

    pool_copy = pltpu.make_async_copy(pool_hbm, pool_ref, local_sem.at[0])
    q_copy = pltpu.make_async_copy(q_hbm, q_ref, local_sem.at[1])
    w_copy = pltpu.make_async_copy(w_hbm, w_ref, local_sem.at[2])
    pool_copy.start()
    w_copy.start()
    q_copy.start()

    barrier = pltpu.get_barrier_semaphore()
    for p in range(1, n):
        pl.semaphore_signal(
            barrier, inc=1, device_id={"pool": (me + p) % n}, device_id_type=MESH
        )
    for d in range(1, serve_n):
        pl.semaphore_signal(
            barrier, inc=1, device_id={"serve": (core + d) % serve_n}, device_id_type=MESH
        )

    lane = lax.broadcasted_iota(jnp.int32, (PAIR, LANES), 1)

    rows = [jnp.int32(0)] * HOT
    seen = jnp.int32(0)
    for j in range(PPAGES):
        mine = table_ref[j] == me
        for r in range(HOT):
            rows[r] = jnp.where(mine & (seen == r), table_ref[PPAGES + j], rows[r])
        seen = seen + jnp.where(mine, 1, 0)

    pool_copy.wait()

    def widen(u, carry):
        for k in range(PAIR_ROWS):
            at = pl.multiple_of(u * PAIR_ROWS * LANES, LANES) + k * LANES
            to = pl.multiple_of(u * PAIR_ROWS * SHELF, SHELF) + k * SHELF
            poolf_ref[pl.ds(to, SLOTS), :] = pool_ref[:, pl.ds(at, LANES)].astype(jnp.float32)
        return carry

    lax.fori_loop(0, PAIR, widen, 0)

    def pick(u, carry):
        for r in range(HOT):
            for k in range(PAIR_ROWS):
                flat_ref[pl.ds(r * FLAT + u * PAIR_ROWS + k, 1), :] = poolf_ref[
                    pl.ds((u * PAIR_ROWS + k) * SHELF + rows[r], 1), :]
        return carry

    lax.fori_loop(0, PAIR, pick, 0)

    def halves(ref, start, count, lane):
        parts = [ref[pl.ds(start + k, count, stride=PAIR_ROWS), :] for k in range(PAIR_ROWS)]
        turned = [pltpu.roll(part, ROPE, 1) for part in parts[4:]]
        odd = [jnp.where(lane < ROPE, turned[c], turned[c + 1]) for c in range(4)]
        return parts, odd, turned[4]

    for r in range(HOT):
        parts, odd, _ = halves(flat_ref, r * FLAT, PAIR, lane)
        for c in range(4):
            at = slice(c * LANES, (c + 1) * LANES)
            lat_ref[0, 0, r * PAGE:r * PAGE + PAIR, at] = parts[c].astype(jnp.bfloat16)
            lat_ref[0, 0, r * PAGE + PAIR:(r + 1) * PAGE, at] = odd[c].astype(jnp.bfloat16)
        rope_ref[0, 0, r * PAIR:(r + 1) * PAIR, :] = jnp.where(
            lane < ROPE, parts[4], parts[8]).astype(jnp.bfloat16)

    owner_of = owners_ref[...]
    index = lax.broadcasted_iota(jnp.int32, (1, LANES), 1)
    held = jnp.clip(table_ref[2 * PPAGES + 2 * NEWP] - PAGE * index, 0, PAGE).astype(jnp.float32)
    named = owner_of == lax.broadcasted_iota(jnp.int32, (n, LANES), 0)
    before = (
        lax.broadcasted_iota(jnp.int32, (LANES, LANES), 0)
        < lax.broadcasted_iota(jnp.int32, (LANES, LANES), 1)
    )
    rank = jnp.dot(
        jnp.where(named, 1.0, 0.0).astype(jnp.bfloat16),
        jnp.where(before, 1.0, 0.0).astype(jnp.bfloat16),
        preferred_element_type=jnp.float32,
    )
    for r in range(HOT):
        count = jnp.sum(
            jnp.where(named & (rank == r), jnp.broadcast_to(held, (n, LANES)), 0.0),
            axis=1, keepdims=True,
        )
        count_ref[r] = jnp.broadcast_to(count, (n, LANES))

    raws_ref[pl.ds(me, 1)] = raw_ref[...][None]
    w_copy.wait()
    wg_ref[pl.ds(core, 1)] = w_ref[...][None]

    pl.semaphore_wait(barrier, n - 1 + serve_n - 1)

    started = []

    def send(src, dst, send_sem, recv_sem, device_id):
        copy = pltpu.make_async_remote_copy(
            src_ref=src, dst_ref=dst, send_sem=send_sem, recv_sem=recv_sem,
            device_id=device_id, device_id_type=MESH,
        )
        copy.start()
        started.append(copy)
        return copy

    order = []
    for d in range(1, depth // 2 + 1):
        order.append(d)
        if depth - d != d:
            order.append(depth - d)
    planes = [0] + order

    def base_of(d):
        return ((z - d + depth) % depth) * 4

    owners = {}
    for d in planes:
        base = base_of(d)
        owners[d, 0] = base + y * 2 + x
        owners[d, 1] = base + y * 2 + (1 - x)
        owners[d, 2] = base + (1 - y) * 2 + x
        owners[d, 3] = base + (1 - y) * 2 + (1 - x)

    def views(d, place, h):
        return (
            lat_ref.at[d, place, pl.ds(h * BLOCK // 2, BLOCK // 2)],
            rope_ref.at[d, place, pl.ds(h * BLOCK // 4, BLOCK // 4)],
        )

    arrivals = {}
    issued = {(0, 0)}

    def pass_on(src, dst, h, sends, recvs, d, slot, there):
        copies = []
        for part, (a, b) in enumerate(zip(views(*src, h), views(*dst, h))):
            copies.append(send(
                a, b, sends.at[d, slot, part], recvs.at[d, slot, part], {"pool": there}))
        arrivals[dst + (h,)] = copies
        issued.add(dst)

    def take(key):
        for copy in arrivals.pop(key, ()):
            copy.wait_recv()

    raw_copies = [
        send(raw_ref, raws_ref.at[me], r_send.at[p], r_recv.at[p], {"pool": (me + p) % n})
        for p in range(1, n)
    ]

    def spread(d, h):
        pass_on((d, 0), (d, 1), h, x_send, x_recv, d, h, x_peer)
        pass_on((d, 0), (d, 2), 1 - h, y_send, y_recv, d, 1 - h, y_peer)

    def forward(d):
        take((d, 1, 0))
        pass_on((d, 1), (d, 3), 0, y_send, y_recv, d, 2, y_peer)
        take((d, 2, 1))
        pass_on((d, 2), (d, 3), 1, x_send, x_recv, d, 2, x_peer)

    for h in range(2):
        spread(0, h)
    for d in order:
        there = ((z + d) % depth) * 4 + y * 2 + x
        for h in range(2):
            copies = []
            for part, (a, b) in enumerate(zip(views(0, 0, h), views(d, 0, h))):
                copies.append(send(
                    a, b, z_send.at[d, h, part], z_recv.at[d, h, part], {"pool": there}))
            arrivals[d, 0, h] = copies
            issued.add((d, 0))
    w_copies = [
        send(w_ref, wg_ref.at[core], w_send.at[d], w_recv.at[d], {"serve": (core + d) % serve_n})
        for d in range(1, serve_n)
    ]

    def advance(d):
        take((d, 0, 0))
        take((d, 0, 1))
        for h in range(2):
            spread(d, h)

    q_copy.wait()
    unit = jnp.where(
        lax.broadcasted_iota(jnp.int32, (SUF, WIDE - LAT), 1) == 0, 1.0, 0.0
    ).astype(jnp.bfloat16)
    for h in range(heads):
        qs_ref[h * SUF:(h + 1) * SUF, :] = jnp.concatenate(
            [q_ref[:, h * LAT:(h + 1) * LAT], unit], axis=1
        )

    def unpack(place, d, at):
        for r in range(HOT):
            rope = rope_ref[d, place, r * PAIR:(r + 1) * PAIR, :].astype(jnp.float32)
            count = count_ref[r, pl.ds(owners[d, place], 1), :]
            turned = pltpu.roll(rope, ROPE, 1)
            line = lax.broadcasted_iota(jnp.int32, (PAIR, LANES), 0).astype(jnp.float32)
            for k, values in enumerate((rope, turned)):
                absent = (lane == ROPE) & (2.0 * line + k >= count)
                tile = jnp.where(lane < ROPE, values, jnp.where(absent, masked_score, 0.0))
                kr_ref[at + r * PAGE + k * PAIR:at + r * PAGE + (k + 1) * PAIR, :] = tile.astype(
                    jnp.bfloat16)

    blocks = [(0, 0), (0, 1), (0, 2)]
    for k, d in enumerate(order):
        blocks += [(d, 0), (d, 1), (d, 2)]
        if k + 1 < len(order):
            blocks.append((planes[k], 3))
    blocks += [(planes[-2], 3), (planes[-1], 3)] if depth > 1 else [(0, 3)]
    pages = [(i, d, place, r) for i, (d, place) in enumerate(blocks) for r in range(HOT)]
    total = len(pages)
    cuts = [8]
    while total - cuts[-1] > 16:
        cuts.append(cuts[-1] + 12)
    cuts += [cuts[-1] + (total - cuts[-1]) // 2, total]
    chunks = [pages[a:b] for a, b in zip([0] + cuts[:-1], cuts)]

    tiles = heads * SUF // TILE

    def loader(chunk):
        def latents(first, count):
            return jnp.concatenate(
                [lat_ref[d, place, r * PAGE:(r + 1) * PAGE, :]
                 for _, d, place, r in chunk[first // PAGE:(first + count) // PAGE]], axis=0)

        def keys(first, count):
            at = (chunk[0][0] * HOT + chunk[0][3]) * PAGE + first
            return jnp.concatenate([latents(first, count), kr_ref[at:at + count, :]], axis=1)

        return latents, keys, len(chunk) * PAGE

    def suffix_loader():
        return (
            lambda first, count: sfx_ref[first:first + count, :VLAT],
            lambda first, count: sfx_ref[first:first + count, :],
            SUF,
        )

    def score(t, load, slot):
        _, keys, size = load
        for at in range(0, size, SUB):
            s_ref[slot, :, at:at + SUB] = lax.dot_general(
                qs_ref[t * TILE:(t + 1) * TILE, :], keys(at, SUB), contract_last,
                preferred_element_type=jnp.float32,
            )

    def absorb(t, load, slot, first, causal):
        latents, _, size = load
        rows = slice(t * TILE, (t + 1) * TILE)
        strips = [s_ref[slot, :, c * LANES:(c + 1) * LANES] for c in range(size // LANES)]
        if causal:
            row = lax.broadcasted_iota(jnp.int32, (TILE, LANES), 0) % SUF
            col = lax.broadcasted_iota(jnp.int32, (TILE, LANES), 1)
            for c in range(size // LANES):
                token = c * LANES + col
                token = jnp.where(token < SUF // 2, 2 * token, 2 * token - SUF + 1)
                strips[c] = jnp.where(token <= row, strips[c], masked_score)
        top = strips[0]
        for strip in strips[1:]:
            top = jnp.maximum(top, strip)
        top = jnp.broadcast_to(jnp.max(top, axis=1, keepdims=True), (TILE, LANES))
        if not first:
            earlier = top_ref[rows, :]
            top = jnp.maximum(top, earlier)
        shift = top * exp2_scale
        weights = []
        added = None
        for strip in strips:
            weight = jnp.exp2(strip * exp2_scale - shift)
            added = weight if added is None else added + weight
            weights.append(weight.astype(jnp.bfloat16))
        mixed = jnp.dot(
            jnp.concatenate(weights, axis=1), latents(0, size), preferred_element_type=jnp.float32
        )
        if not first:
            rescale = jnp.exp2((earlier - top) * exp2_scale)
            added = added + sum_ref[rows, :] * rescale
            mixed = mixed + acc_ref[rows, :] * jnp.concatenate([rescale] * (VLAT // LANES), axis=1)
        top_ref[rows, :] = top
        sum_ref[rows, :] = added
        acc_ref[rows, :] = mixed

    def attend(load, first, causal, between):
        score(0, load, 0)
        for t in range(tiles):
            if t + 1 < tiles:
                score(t + 1, load, (t + 1) % 2)
            absorb(t, load, t % 2, first, causal)
            between(t)

    pending = []
    for k, d in enumerate(planes):
        pending.append(functools.partial(forward, d))
        if k + 1 < depth:
            pending.append(functools.partial(advance, planes[k + 1]))

    def communicate(steps):
        for _ in range(min(steps, len(pending))):
            pending.pop(0)()

    for copy in raw_copies:
        copy.wait_recv()
    for o in range(n):
        rawf_ref[o * raw_rows:(o + 1) * raw_rows, :] = raws_ref[o].astype(jnp.float32)
    wide_lane = lax.broadcasted_iota(jnp.int32, (SUF // 2, LANES), 1)
    parts, odd, last = halves(rawf_ref, 0, SUF // 2, wide_lane)
    for c in range(4):
        at = slice(c * LANES, (c + 1) * LANES)
        sfx_ref[:SUF // 2, at] = parts[c].astype(jnp.bfloat16)
        sfx_ref[SUF // 2:, at] = odd[c].astype(jnp.bfloat16)
    for half, values in enumerate((parts[4], last)):
        sfx_ref[half * SUF // 2:(half + 1) * SUF // 2, VLAT:] = jnp.where(
            wide_lane < ROPE, values, 0.0).astype(jnp.bfloat16)

    attend(suffix_loader(), True, True, lambda t: None)
    communicate(1)

    page = jnp.int32(0)
    slot = jnp.int32(-1)
    for m in range(NEWP):
        mine = table_ref[2 * PPAGES + m] == me
        page = jnp.where(mine, m, page)
        slot = jnp.where(mine, table_ref[2 * PPAGES + NEWP + m], slot)
    chosen = lax.broadcasted_iota(jnp.int32, (SLOTS, LANES), 0) == slot

    def write(u, carry):
        for k in range(PAIR_ROWS):
            at = pl.multiple_of(u * PAIR_ROWS * LANES, LANES) + k * LANES
            fresh = rawf_ref[pl.ds(page * FLAT + u * PAIR_ROWS + k, 1), :]
            to = pl.multiple_of(u * PAIR_ROWS * SHELF, SHELF) + k * SHELF
            kept = poolf_ref[pl.ds(to, SLOTS), :]
            new_ref[:, pl.ds(at, LANES)] = jnp.where(chosen, fresh, kept).astype(jnp.bfloat16)
        return carry

    lax.fori_loop(0, PAIR, write, 0)

    ready = 0
    for k, chunk in enumerate(chunks):
        while ready <= chunk[-1][0]:
            d, place = blocks[ready]
            while (d, place) not in issued:
                communicate(1)
            take((d, place, 0))
            take((d, place, 1))
            unpack(place, d, ready * BLOCK)
            ready += 1
        attend(loader(chunk), False, False, lambda t: communicate(1) if t % 2 else None)
    for copy in w_copies:
        copy.wait_recv()
    for h in range(heads):
        rows = slice(h * SUF, (h + 1) * SUF)
        mixed = (acc_ref[rows, :] / jnp.sum(sum_ref[rows, :], axis=1, keepdims=True)).astype(
            jnp.bfloat16)
        out_ref[:, h * VHEAD:(h + 1) * VHEAD] = jnp.dot(
            mixed, wg_ref[:, h].reshape(VLAT, VHEAD), preferred_element_type=jnp.float32
        ).astype(jnp.bfloat16)
    for copy in started:
        copy.wait_send()


def fused(n, serve_n, table, owners, raw, pages, queries, w):
    depth = n // 4
    heads = queries.shape[1] // LAT
    dma = pltpu.SemaphoreType.DMA
    vmem = pl.BlockSpec(memory_space=pltpu.VMEM)
    hbm = pl.BlockSpec(memory_space=pl.ANY)
    bf16, f32 = jnp.bfloat16, jnp.float32
    rows = heads * SUF
    return pl.pallas_call(
        functools.partial(fused_kernel, n, serve_n),
        out_shape=(
            jax.ShapeDtypeStruct((SUF, heads * VHEAD), bf16),
            jax.ShapeDtypeStruct(pages.shape, bf16),
        ),
        in_specs=[pl.BlockSpec(memory_space=pltpu.SMEM), vmem, vmem, hbm, hbm, hbm],
        out_specs=(vmem, vmem),
        scratch_shapes=[
            pltpu.VMEM(pages.shape, bf16),
            pltpu.VMEM((FLAT * SHELF, LANES), f32),
            pltpu.VMEM((HOT * FLAT, LANES), f32),
            pltpu.VMEM(queries.shape, bf16),
            pltpu.VMEM(w.shape, bf16),
            pltpu.VMEM((serve_n,) + w.shape, bf16),
            pltpu.VMEM((rows, WIDE), bf16),
            pltpu.VMEM((depth, 4, BLOCK, VLAT), bf16),
            pltpu.VMEM((depth, 4, BLOCK // 2, LANES), bf16),
            pltpu.VMEM((n * BLOCK, LANES), bf16),
            pltpu.VMEM((n,) + raw.shape, bf16),
            pltpu.VMEM((n * raw.shape[0], LANES), f32),
            pltpu.VMEM((SUF, WIDE), bf16),
            pltpu.VMEM((HOT, n, LANES), f32),
            pltpu.VMEM((2, TILE, 12 * PAGE), f32),
            pltpu.VMEM((rows, VLAT), f32),
            pltpu.VMEM((rows, LANES), f32),
            pltpu.VMEM((rows, LANES), f32),
            dma((3,)),
            dma((depth, 2, 2)), dma((depth, 2, 2)),
            dma((depth, 3, 2)), dma((depth, 3, 2)),
            dma((depth, 3, 2)), dma((depth, 3, 2)),
            dma((serve_n,)), dma((serve_n,)),
            dma((n,)), dma((n,)),
        ],
        compiler_params=pltpu.CompilerParams(
            collective_id=0, has_side_effects=True, vmem_limit_bytes=56 * 1024 * 1024
        ),
        name="fused",
    )(table, owners, raw, pages, queries, w)


def local(n, serve_n, queries, new_latent, pool, page_owner, page_slot, new_owner, new_slot,
          prefix_len, w_uv):
    table = jnp.concatenate([page_owner[0], page_slot[0], new_owner[0], new_slot[0], prefix_len])
    owners = jnp.pad(page_owner, ((0, 0), (0, LANES - PPAGES)), constant_values=-1)
    raw = new_latent.reshape(-1, LANES)
    attended, updated = fused(n, serve_n, table, owners, raw, pool[0], queries[0], w_uv)
    return (attended[None], updated[None])


def solution(mesh):
    in_specs = (
        P("serve", None, "pool"),
        P("serve", "pool"),
        P("serve", "pool", None),
        P("serve", None),
        P("serve", None),
        P("serve", None),
        P("serve", None),
        P("serve"),
        P("pool", "serve", None),
    )
    out_specs = (P("serve", None, "pool"), P("serve", "pool", None))
    body = functools.partial(local, mesh.shape["pool"], mesh.shape["serve"])
    return jax.shard_map(body, mesh=mesh, in_specs=in_specs, out_specs=out_specs, check_vma=False)
```

```python
import functools

import jax
import jax.numpy as jnp
from jax import lax
from jax.experimental import pallas as pl
from jax.experimental.pallas import tpu as pltpu
from jax.sharding import PartitionSpec as P

VLAT = 512
VHEAD = 128
PAGE = 64
SUF = 256
HOT = 3
LAT = 576
PPAGES = 32
NEWP = 4
SLOTS = 12

LANES = 128
ROPE = LAT - VLAT
WIDE = VLAT + LANES
PAIR = PAGE // 2
PAIR_ROWS = 2 * LAT // LANES
FLAT = PAGE * LAT // LANES
BLOCK = HOT * PAGE
SHELF = 16
TILE = 512
SUB = 256

softmax_scale = 192.0 ** (-0.5)
masked_score = -1e30
exp2_scale = softmax_scale * 1.4426950408889634

MESH = pl.DeviceIdType.MESH
contract_last = (((1,), (1,)), ((), ()))


def fused_kernel(n, serve_n, owner_hbm, slot_hbm, new_owner_hbm, new_slot_hbm, len_ref, fresh_hbm,
                 pool_hbm, q_hbm, w_hbm, out_ref, new_ref,
                 owner_ref, slot_ref, new_owner_ref, new_slot_ref, named_ref, fresh_ref,
                 pool_ref, poolf_ref, flat_ref, own_ref, raw_ref, q_ref, w_ref, wg_ref, qs_ref,
                 lat_ref, rope_ref, kr_ref, raws_ref, rawf_ref, sfx_ref, count_ref, s_ref, acc_ref,
                 top_ref, sum_ref, local_sem, z_send, z_recv, x_send, x_recv, y_send, y_recv,
                 c_send, w_send, w_recv, rz_send, rz_recv, r_send, r_recv):
    depth = n // 4
    heads = q_ref.shape[1] // LAT
    raw_rows = raw_ref.shape[0]
    me = lax.axis_index("pool")
    core = lax.axis_index("serve")
    x = me % 2
    y = (me // 2) % 2
    z = me // 4
    x_peer = z * 4 + y * 2 + (1 - x)
    y_peer = z * 4 + (1 - y) * 2 + x
    far_peer = z * 4 + (1 - y) * 2 + (1 - x)
    column = [((z + d) % depth) * 4 + y * 2 + x for d in range(depth)]

    fetches = [
        pltpu.make_async_copy(src, dst, local_sem.at[i])
        for i, (src, dst) in enumerate((
            (owner_hbm, owner_ref), (slot_hbm, slot_ref), (pool_hbm, pool_ref),
            (fresh_hbm, fresh_ref), (w_hbm, w_ref), (q_hbm, q_ref), (owner_hbm, named_ref),
            (new_owner_hbm, new_owner_ref), (new_slot_hbm, new_slot_ref),
        ))
    ]
    for fetch in fetches:
        fetch.start()

    barrier = pltpu.get_barrier_semaphore()
    peers = column[1:] + [x_peer, y_peer, far_peer]
    for there in peers:
        pl.semaphore_signal(barrier, inc=1, device_id={"pool": there}, device_id_type=MESH)
    for d in range(1, serve_n):
        pl.semaphore_signal(
            barrier, inc=1, device_id={"serve": (core + d) % serve_n}, device_id_type=MESH
        )

    lane = lax.broadcasted_iota(jnp.int32, (PAIR, LANES), 1)

    fetches[0].wait()
    fetches[1].wait()
    rows = [jnp.int32(0)] * HOT
    seen = jnp.int32(0)
    for j in range(PPAGES):
        mine = owner_ref[0, j] == me
        for r in range(HOT):
            rows[r] = jnp.where(mine & (seen == r), slot_ref[0, j], rows[r])
        seen = seen + jnp.where(mine, 1, 0)

    fetches[2].wait()

    def widen(u, carry):
        for k in range(PAIR_ROWS):
            at = pl.multiple_of(u * PAIR_ROWS * LANES, LANES) + k * LANES
            to = pl.multiple_of(u * PAIR_ROWS * SHELF, SHELF) + k * SHELF
            poolf_ref[pl.ds(to, SLOTS), :] = pool_ref[:, pl.ds(at, LANES)].astype(jnp.float32)
        return carry

    lax.fori_loop(0, PAIR, widen, 0)

    def pick(u, carry):
        for r in range(HOT):
            for k in range(PAIR_ROWS):
                flat_ref[pl.ds(r * FLAT + u * PAIR_ROWS + k, 1), :] = poolf_ref[
                    pl.ds((u * PAIR_ROWS + k) * SHELF + rows[r], 1), :]
        return carry

    lax.fori_loop(0, PAIR, pick, 0)

    def halves(ref, start, count, lane):
        parts = [ref[pl.ds(start + k, count, stride=PAIR_ROWS), :] for k in range(PAIR_ROWS)]
        turned = [pltpu.roll(part, ROPE, 1) for part in parts[4:]]
        odd = [jnp.where(lane < ROPE, turned[c], turned[c + 1]) for c in range(4)]
        return parts, odd, turned[4]

    for r in range(HOT):
        parts, odd, _ = halves(flat_ref, r * FLAT, PAIR, lane)
        for c in range(4):
            at = slice(c * LANES, (c + 1) * LANES)
            lat_ref[0, 0, r * PAGE:r * PAGE + PAIR, at] = parts[c].astype(jnp.bfloat16)
            lat_ref[0, 0, r * PAGE + PAIR:(r + 1) * PAGE, at] = odd[c].astype(jnp.bfloat16)
        rope_ref[0, 0, r * PAIR:(r + 1) * PAIR, :] = jnp.where(
            lane < ROPE, parts[4], parts[8]).astype(jnp.bfloat16)

    fetches[3].wait()
    for k in range(raw_rows):
        own_ref[k:k + 1, :] = fresh_ref[:, k * LANES:(k + 1) * LANES].astype(jnp.float32)
    raw_ref[...] = own_ref[...].astype(jnp.bfloat16)
    fetches[4].wait()

    pl.semaphore_wait(barrier, len(peers) + serve_n - 1)

    started = []

    def send(src, dst, send_sem, recv_sem, device_id):
        copy = pltpu.make_async_remote_copy(
            src_ref=src, dst_ref=dst, send_sem=send_sem, recv_sem=recv_sem,
            device_id=device_id, device_id_type=MESH,
        )
        copy.start()
        started.append(copy)
        return copy

    order = []
    for d in range(1, depth // 2 + 1):
        order.append(d)
        if depth - d != d:
            order.append(depth - d)
    planes = [0] + order

    def base_of(d):
        return ((z - d + depth) % depth) * 4

    owners = {}
    for d in planes:
        base = base_of(d)
        owners[d, 0] = base + y * 2 + x
        owners[d, 1] = base + y * 2 + (1 - x)
        owners[d, 2] = base + (1 - y) * 2 + x
        owners[d, 3] = base + (1 - y) * 2 + (1 - x)

    def views(d, place, h):
        return (
            lat_ref.at[d, place, pl.ds(h * BLOCK // 2, BLOCK // 2)],
            rope_ref.at[d, place, pl.ds(h * BLOCK // 4, BLOCK // 4)],
        )

    arrivals = {}
    issued = {(0, 0)}

    def pass_on(src, dst, h, sends, recvs, d, slot, there):
        copies = []
        for part, (a, b) in enumerate(zip(views(*src, h), views(*dst, h))):
            copies.append(send(
                a, b, sends.at[d, slot, part], recvs.at[d, slot, part], {"pool": there}))
        arrivals[dst + (h,)] = copies
        issued.add(dst)

    def take(key):
        for copy in arrivals.pop(key, ()):
            copy.wait_recv()

    def spread(d, h):
        pass_on((d, 0), (d, 1), h, x_send, x_recv, d, h, x_peer)
        pass_on((d, 0), (d, 2), 1 - h, y_send, y_recv, d, 1 - h, y_peer)

    def start_if(condition, copies):
        @pl.when(condition)
        def _():
            for copy in copies:
                copy.start()
        guarded.append((condition, copies))

    def halved(src, dst, there, sends, recvs):
        return [
            pltpu.make_async_remote_copy(
                src_ref=a, dst_ref=b, send_sem=sends.at[part], recv_sem=recvs.at[part],
                device_id={"pool": there}, device_id_type=MESH,
            )
            for part, (a, b) in enumerate(zip(src, dst))
        ]

    guarded = []
    near = {1: (z == 0, z < depth - 1), depth - 1: (z == depth - 1, z > 0)}

    def forward(d):
        for place, h, there, sends, recvs in (
            (1, 0, y_peer, y_send, y_recv), (2, 1, x_peer, x_send, x_recv)
        ):
            take((d, place, h))
            if d in near:
                copies = halved(views(d, place, h), views(d, 3, h), there,
                                sends.at[d, 2], recvs.at[d, 2])
                start_if(near[d][0], copies)
                arrivals[d, 3, h] = copies
                issued.add((d, 3))
            else:
                pass_on((d, place), (d, 3), h, sends, recvs, d, 2, there)

    def cross():
        for h, recvs in ((0, y_recv), (1, x_recv)):
            take((0, 3, h))
        for i, d in enumerate(near):
            copies = []
            for h, recvs in ((0, y_recv), (1, x_recv)):
                copies += halved(views(0, 3, h), views(d, 3, h), column[d],
                                 c_send.at[i, h], recvs.at[d, 2])
            start_if(near[d][1], copies)

    raw_column = {
        d: send(raw_ref, raws_ref.at[me], rz_send.at[d], rz_recv.at[d], {"pool": column[d]})
        for d in order
    }
    for h in range(2):
        spread(0, h)
    for d in order:
        for h in range(2):
            copies = []
            for part, (a, b) in enumerate(zip(views(0, 0, h), views(d, 0, h))):
                copies.append(send(
                    a, b, z_send.at[d, h, part], z_recv.at[d, h, part], {"pool": column[d]}))
            arrivals[d, 0, h] = copies
            issued.add((d, 0))

    raw_copies = []

    def pass_raw(d):
        owner = owners[d, 0]
        src = raw_ref if d == 0 else raws_ref.at[owner]
        for i, there in enumerate((x_peer, y_peer, far_peer)):
            raw_copies.append(send(
                src, raws_ref.at[owner], r_send.at[d, i], r_recv.at[d, i], {"pool": there}))

    pass_raw(0)
    w_copies = [
        send(w_ref, wg_ref.at[core], w_send.at[d], w_recv.at[d], {"serve": (core + d) % serve_n})
        for d in range(1, serve_n)
    ]

    def advance(d):
        take((d, 0, 0))
        take((d, 0, 1))
        for h in range(2):
            spread(d, h)

    for fetch in fetches[6:]:
        fetch.wait()
    index = lax.broadcasted_iota(jnp.int32, (1, PPAGES), 1)
    held = jnp.clip(len_ref[0] - PAGE * index, 0, PAGE).astype(jnp.float32)
    named = named_ref[...] == lax.broadcasted_iota(jnp.int32, (n, PPAGES), 0)
    before = (
        lax.broadcasted_iota(jnp.int32, (PPAGES, PPAGES), 0)
        < lax.broadcasted_iota(jnp.int32, (PPAGES, PPAGES), 1)
    )
    rank = jnp.dot(
        jnp.where(named, 1.0, 0.0).astype(jnp.bfloat16),
        jnp.where(before, 1.0, 0.0).astype(jnp.bfloat16),
        preferred_element_type=jnp.float32,
    )
    for r in range(HOT):
        count = jnp.sum(
            jnp.where(named & (rank == r), jnp.broadcast_to(held, (n, PPAGES)), 0.0),
            axis=1, keepdims=True,
        )
        count_ref[r] = jnp.broadcast_to(count, (n, LANES))

    raws_ref[pl.ds(me, 1)] = raw_ref[...][None]
    wg_ref[pl.ds(core, 1)] = w_ref[...][None]
    fetches[5].wait()
    unit = jnp.where(
        lax.broadcasted_iota(jnp.int32, (SUF, WIDE - LAT), 1) == 0, 1.0, 0.0
    ).astype(jnp.bfloat16)
    for h in range(heads):
        qs_ref[h * SUF:(h + 1) * SUF, :] = jnp.concatenate(
            [q_ref[:, h * LAT:(h + 1) * LAT], unit], axis=1
        )

    def unpack(place, d, at):
        for r in range(HOT):
            rope = rope_ref[d, place, r * PAIR:(r + 1) * PAIR, :].astype(jnp.float32)
            count = count_ref[r, pl.ds(owners[d, place], 1), :]
            turned = pltpu.roll(rope, ROPE, 1)
            line = lax.broadcasted_iota(jnp.int32, (PAIR, LANES), 0).astype(jnp.float32)
            for k, values in enumerate((rope, turned)):
                absent = (lane == ROPE) & (2.0 * line + k >= count)
                tile = jnp.where(lane < ROPE, values, jnp.where(absent, masked_score, 0.0))
                kr_ref[at + r * PAGE + k * PAIR:at + r * PAGE + (k + 1) * PAIR, :] = tile.astype(
                    jnp.bfloat16)

    for d in order:
        raw_column[d].wait_recv()
        pass_raw(d)

    blocks = [(0, 0), (0, 1), (0, 2)]
    for k, d in enumerate(order):
        blocks += [(d, 0), (d, 1), (d, 2)]
        if k == 0:
            blocks.append((0, 3))
    blocks += [(d, 3) for d in order]
    pages = [(i, d, place, r) for i, (d, place) in enumerate(blocks) for r in range(HOT)]
    total = len(pages)
    cuts = [8]
    while total - cuts[-1] > 16:
        cuts.append(cuts[-1] + 12)
    cuts += [cuts[-1] + (total - cuts[-1]) // 2, total]
    chunks = [pages[a:b] for a, b in zip([0] + cuts[:-1], cuts)]

    tiles = heads * SUF // TILE

    def loader(chunk):
        def latents(first, count):
            return jnp.concatenate(
                [lat_ref[d, place, r * PAGE:(r + 1) * PAGE, :]
                 for _, d, place, r in chunk[first // PAGE:(first + count) // PAGE]], axis=0)

        def keys(first, count):
            at = (chunk[0][0] * HOT + chunk[0][3]) * PAGE + first
            return jnp.concatenate([latents(first, count), kr_ref[at:at + count, :]], axis=1)

        return latents, keys, len(chunk) * PAGE

    def suffix_loader():
        return (
            lambda first, count: sfx_ref[first:first + count, :VLAT],
            lambda first, count: sfx_ref[first:first + count, :],
            SUF,
        )

    def score(t, load, slot):
        _, keys, size = load
        for at in range(0, size, SUB):
            s_ref[slot, :, at:at + SUB] = lax.dot_general(
                qs_ref[t * TILE:(t + 1) * TILE, :], keys(at, SUB), contract_last,
                preferred_element_type=jnp.float32,
            )

    def absorb(t, load, slot, first, causal):
        latents, _, size = load
        rows = slice(t * TILE, (t + 1) * TILE)
        strips = [s_ref[slot, :, c * LANES:(c + 1) * LANES] for c in range(size // LANES)]
        if causal:
            row = lax.broadcasted_iota(jnp.int32, (TILE, LANES), 0) % SUF
            col = lax.broadcasted_iota(jnp.int32, (TILE, LANES), 1)
            for c in range(size // LANES):
                token = c * LANES + col
                token = jnp.where(token < SUF // 2, 2 * token, 2 * token - SUF + 1)
                strips[c] = jnp.where(token <= row, strips[c], masked_score)
        top = strips[0]
        for strip in strips[1:]:
            top = jnp.maximum(top, strip)
        top = jnp.broadcast_to(jnp.max(top, axis=1, keepdims=True), (TILE, LANES))
        if not first:
            earlier = top_ref[rows, :]
            top = jnp.maximum(top, earlier)
        shift = top * exp2_scale
        weights = []
        added = None
        for strip in strips:
            weight = jnp.exp2(strip * exp2_scale - shift)
            added = weight if added is None else added + weight
            weights.append(weight.astype(jnp.bfloat16))
        mixed = jnp.dot(
            jnp.concatenate(weights, axis=1), latents(0, size), preferred_element_type=jnp.float32
        )
        if not first:
            rescale = jnp.exp2((earlier - top) * exp2_scale)
            added = added + sum_ref[rows, :] * rescale
            mixed = mixed + acc_ref[rows, :] * jnp.concatenate([rescale] * (VLAT // LANES), axis=1)
        top_ref[rows, :] = top
        sum_ref[rows, :] = added
        acc_ref[rows, :] = mixed

    def attend(load, first, causal, between):
        score(0, load, 0)
        for t in range(tiles):
            if t + 1 < tiles:
                score(t + 1, load, (t + 1) % 2)
            absorb(t, load, t % 2, first, causal)
            between(t)

    pending = [functools.partial(forward, 0)]
    for k, d in enumerate(order):
        pending.append(functools.partial(advance, d))
        if k == 0:
            pending.append(cross)
        pending.append(functools.partial(forward, d))

    def communicate(steps):
        for _ in range(min(steps, len(pending))):
            pending.pop(0)()

    def suffix():
        for copy in raw_copies:
            copy.wait_recv()
        for o in range(n):
            rawf_ref[o * raw_rows:(o + 1) * raw_rows, :] = raws_ref[o].astype(jnp.float32)
        wide_lane = lax.broadcasted_iota(jnp.int32, (SUF // 2, LANES), 1)
        parts, odd, last = halves(rawf_ref, 0, SUF // 2, wide_lane)
        for c in range(4):
            at = slice(c * LANES, (c + 1) * LANES)
            sfx_ref[:SUF // 2, at] = parts[c].astype(jnp.bfloat16)
            sfx_ref[SUF // 2:, at] = odd[c].astype(jnp.bfloat16)
        for half, values in enumerate((parts[4], last)):
            sfx_ref[half * SUF // 2:(half + 1) * SUF // 2, VLAT:] = jnp.where(
                wide_lane < ROPE, values, 0.0).astype(jnp.bfloat16)

        attend(suffix_loader(), False, True, lambda t: communicate(1) if t % 2 else None)

        page = jnp.int32(0)
        slot = jnp.int32(-1)
        for m in range(NEWP):
            mine = new_owner_ref[0, m] == me
            page = jnp.where(mine, m, page)
            slot = jnp.where(mine, new_slot_ref[0, m], slot)
        chosen = lax.broadcasted_iota(jnp.int32, (SLOTS, LANES), 0) == slot

        def write(u, carry):
            for k in range(PAIR_ROWS):
                at = pl.multiple_of(u * PAIR_ROWS * LANES, LANES) + k * LANES
                fresh = rawf_ref[pl.ds(page * FLAT + u * PAIR_ROWS + k, 1), :]
                to = pl.multiple_of(u * PAIR_ROWS * SHELF, SHELF) + k * SHELF
                kept = poolf_ref[pl.ds(to, SLOTS), :]
                new_ref[:, pl.ds(at, LANES)] = jnp.where(chosen, fresh, kept).astype(jnp.bfloat16)
            return carry

        lax.fori_loop(0, PAIR, write, 0)

    steps = [{0: 1, 2: 1}, {3: 1}, {0: 1, 3: 1}]

    communicate(1)
    ready = 0
    for k, chunk in enumerate(chunks):
        while ready <= chunk[-1][0]:
            d, place = blocks[ready]
            while (d, place) not in issued:
                communicate(1)
            take((d, place, 0))
            take((d, place, 1))
            unpack(place, d, ready * BLOCK)
            ready += 1
        when = steps[k] if k < len(steps) else {}
        attend(loader(chunk), k == 0, False, lambda t: communicate(when.get(t, 0)))
        if k == 0:
            suffix()
    for copy in w_copies:
        copy.wait_recv()
    for h in range(heads):
        rows = slice(h * SUF, (h + 1) * SUF)
        share = 1.0 / jnp.sum(sum_ref[rows, :], axis=1, keepdims=True)
        mixed = (acc_ref[rows, :] * share).astype(jnp.bfloat16)
        out_ref[:, h * VHEAD:(h + 1) * VHEAD] = jnp.dot(
            mixed, wg_ref[:, h].reshape(VLAT, VHEAD), preferred_element_type=jnp.float32
        ).astype(jnp.bfloat16)
    for copy in started:
        copy.wait_send()
    for condition, copies in guarded:
        @pl.when(condition)
        def _(copies=copies):
            for copy in copies:
                copy.wait_send()


def fused(n, serve_n, tables, length, *arrays):
    fresh, pages, queries, w = arrays
    depth = n // 4
    heads = queries.shape[1] // LAT
    raw = (fresh.shape[1] // LANES, LANES)
    dma = pltpu.SemaphoreType.DMA
    vmem = pl.BlockSpec(memory_space=pltpu.VMEM)
    hbm = pl.BlockSpec(memory_space=pltpu.HBM)
    bf16, f32, i32 = jnp.bfloat16, jnp.float32, jnp.int32
    rows = heads * SUF
    return pl.pallas_call(
        functools.partial(fused_kernel, n, serve_n),
        out_shape=(
            jax.ShapeDtypeStruct((SUF, heads * VHEAD), bf16),
            jax.ShapeDtypeStruct(pages.shape, bf16),
        ),
        in_specs=[hbm] * len(tables) + [pl.BlockSpec(memory_space=pltpu.SMEM)] + [hbm] * 4,
        out_specs=(vmem, vmem),
        scratch_shapes=[pltpu.SMEM(table.shape, i32) for table in tables] + [
            pltpu.VMEM(tables[0].shape, i32),
            pltpu.VMEM(fresh.shape, bf16),
            pltpu.VMEM(pages.shape, bf16),
            pltpu.VMEM((FLAT * SHELF, LANES), f32),
            pltpu.VMEM((HOT * FLAT, LANES), f32),
            pltpu.VMEM(raw, f32),
            pltpu.VMEM(raw, bf16),
            pltpu.VMEM(queries.shape, bf16),
            pltpu.VMEM(w.shape, bf16),
            pltpu.VMEM((serve_n,) + w.shape, bf16),
            pltpu.VMEM((rows, WIDE), bf16),
            pltpu.VMEM((depth, 4, BLOCK, VLAT), bf16),
            pltpu.VMEM((depth, 4, BLOCK // 2, LANES), bf16),
            pltpu.VMEM((n * BLOCK, LANES), bf16),
            pltpu.VMEM((n,) + raw, bf16),
            pltpu.VMEM((n * raw[0], LANES), f32),
            pltpu.VMEM((SUF, WIDE), bf16),
            pltpu.VMEM((HOT, n, LANES), f32),
            pltpu.VMEM((2, TILE, 12 * PAGE), f32),
            pltpu.VMEM((rows, VLAT), f32),
            pltpu.VMEM((rows, LANES), f32),
            pltpu.VMEM((rows, LANES), f32),
            dma((9,)),
            dma((depth, 2, 2)), dma((depth, 2, 2)),
            dma((depth, 3, 2)), dma((depth, 3, 2)),
            dma((depth, 3, 2)), dma((depth, 3, 2)),
            dma((2, 2, 2)),
            dma((serve_n,)), dma((serve_n,)),
            dma((depth,)), dma((depth,)),
            dma((depth, 3)), dma((depth, 3)),
        ],
        compiler_params=pltpu.CompilerParams(
            collective_id=0, has_side_effects=True, vmem_limit_bytes=36 * 1024 * 1024
        ),
        name="fused",
    )(*(pltpu.with_memory_space_constraint(t, pltpu.HBM) for t in tables), length,
      *(pltpu.with_memory_space_constraint(t, pltpu.HBM) for t in arrays))


def local(n, serve_n, queries, new_latent, pool, page_owner, page_slot, new_owner, new_slot,
          prefix_len, w_uv):
    tables = (page_owner, page_slot, new_owner, new_slot)
    attended, updated = fused(n, serve_n, tables, prefix_len, new_latent, pool[0], queries[0], w_uv)
    return (attended[None], updated[None])


def solution(mesh):
    in_specs = (
        P("serve", None, "pool"),
        P("serve", "pool"),
        P("serve", "pool", None),
        P("serve", None),
        P("serve", None),
        P("serve", None),
        P("serve", None),
        P("serve"),
        P("pool", "serve", None),
    )
    out_specs = (P("serve", None, "pool"), P("serve", "pool", None))
    body = functools.partial(local, mesh.shape["pool"], mesh.shape["serve"])
    return jax.shard_map(body, mesh=mesh, in_specs=in_specs, out_specs=out_specs, check_vma=False)
```

```python
import functools

import jax
import jax.numpy as jnp
from jax import lax
from jax.experimental import pallas as pl
from jax.experimental.pallas import tpu as pltpu
from jax.sharding import PartitionSpec as P

VLAT = 512
VHEAD = 128
PAGE = 64
SUF = 256
HOT = 3
LAT = 576
PPAGES = 32
NEWP = 4
SLOTS = 12

LANES = 128
ROPE = LAT - VLAT
WIDE = VLAT + LANES
PAIR = PAGE // 2
PAIR_ROWS = 2 * LAT // LANES
FLAT = PAGE * LAT // LANES
BLOCK = HOT * PAGE
SHELF = 16
TILE = 512
SUB = 256

softmax_scale = 192.0 ** (-0.5)
masked_score = -1e30
exp2_scale = softmax_scale * 1.4426950408889634

MESH = pl.DeviceIdType.MESH
contract_last = (((1,), (1,)), ((), ()))


def fused_kernel(n, serve_n, owner_hbm, slot_hbm, new_owner_hbm, new_slot_hbm, len_ref, fresh_hbm,
                 pool_hbm, q_hbm, w_hbm, out_ref, new_ref,
                 owner_ref, slot_ref, new_owner_ref, new_slot_ref, named_ref, fresh_ref,
                 pool_ref, poolf_ref, flat_ref, own_ref, raw_ref, q_ref, w_ref, wg_ref, qs_ref,
                 lat_ref, rope_ref, kr_ref, raws_ref, rawf_ref, sfx_ref, count_ref, s_ref, acc_ref,
                 top_ref, sum_ref, local_sem, z_send, z_recv, x_send, x_recv, y_send, y_recv,
                 c_send, w_send, w_recv, rz_send, rz_recv, r_send, r_recv):
    depth = n // 4
    heads = q_ref.shape[1] // LAT
    raw_rows = raw_ref.shape[0]
    me = lax.axis_index("pool")
    core = lax.axis_index("serve")
    x = me % 2
    y = (me // 2) % 2
    z = me // 4
    x_peer = z * 4 + y * 2 + (1 - x)
    y_peer = z * 4 + (1 - y) * 2 + x
    far_peer = z * 4 + (1 - y) * 2 + (1 - x)
    column = [((z + d) % depth) * 4 + y * 2 + x for d in range(depth)]

    fetches = [
        pltpu.make_async_copy(src, dst, local_sem.at[i])
        for i, (src, dst) in enumerate((
            (owner_hbm, owner_ref), (slot_hbm, slot_ref), (pool_hbm, pool_ref),
            (fresh_hbm, fresh_ref), (w_hbm, w_ref), (q_hbm, q_ref), (owner_hbm, named_ref),
            (new_owner_hbm, new_owner_ref), (new_slot_hbm, new_slot_ref),
        ))
    ]
    for fetch in fetches:
        fetch.start()

    barrier = pltpu.get_barrier_semaphore()
    peers = column[1:] + [x_peer, y_peer, far_peer]
    for there in peers:
        pl.semaphore_signal(barrier, inc=1, device_id={"pool": there}, device_id_type=MESH)
    for d in range(1, serve_n):
        pl.semaphore_signal(
            barrier, inc=1, device_id={"serve": (core + d) % serve_n}, device_id_type=MESH
        )

    lane = lax.broadcasted_iota(jnp.int32, (PAIR, LANES), 1)

    fetches[0].wait()
    fetches[1].wait()
    rows = [jnp.int32(0)] * HOT
    seen = jnp.int32(0)
    for j in range(PPAGES):
        mine = owner_ref[0, j] == me
        for r in range(HOT):
            rows[r] = jnp.where(mine & (seen == r), slot_ref[0, j], rows[r])
        seen = seen + jnp.where(mine, 1, 0)

    fetches[2].wait()

    def widen(u, carry):
        for k in range(PAIR_ROWS):
            at = pl.multiple_of(u * PAIR_ROWS * LANES, LANES) + k * LANES
            to = pl.multiple_of(u * PAIR_ROWS * SHELF, SHELF) + k * SHELF
            poolf_ref[pl.ds(to, SLOTS), :] = pool_ref[:, pl.ds(at, LANES)].astype(jnp.float32)
        return carry

    lax.fori_loop(0, PAIR, widen, 0)

    def pick(u, carry):
        for r in range(HOT):
            for k in range(PAIR_ROWS):
                flat_ref[pl.ds(r * FLAT + u * PAIR_ROWS + k, 1), :] = poolf_ref[
                    pl.ds((u * PAIR_ROWS + k) * SHELF + rows[r], 1), :]
        return carry

    lax.fori_loop(0, PAIR, pick, 0)

    def halves(ref, start, count, lane):
        parts = [ref[pl.ds(start + k, count, stride=PAIR_ROWS), :] for k in range(PAIR_ROWS)]
        turned = [pltpu.roll(part, ROPE, 1) for part in parts[4:]]
        odd = [jnp.where(lane < ROPE, turned[c], turned[c + 1]) for c in range(4)]
        return parts, odd, turned[4]

    for r in range(HOT):
        parts, odd, _ = halves(flat_ref, r * FLAT, PAIR, lane)
        for c in range(4):
            at = slice(c * LANES, (c + 1) * LANES)
            lat_ref[z, 0, r * PAGE:r * PAGE + PAIR, at] = parts[c].astype(jnp.bfloat16)
            lat_ref[z, 0, r * PAGE + PAIR:(r + 1) * PAGE, at] = odd[c].astype(jnp.bfloat16)
        rope_ref[z, 0, r * PAIR:(r + 1) * PAIR, :] = jnp.where(
            lane < ROPE, parts[4], parts[8]).astype(jnp.bfloat16)

    fetches[3].wait()
    for k in range(raw_rows):
        own_ref[k:k + 1, :] = fresh_ref[:, k * LANES:(k + 1) * LANES].astype(jnp.float32)
    raw_ref[...] = own_ref[...].astype(jnp.bfloat16)
    pl.semaphore_wait(barrier, len(peers) + serve_n - 1)

    started = []

    def send(src, dst, send_sem, recv_sem, device_id):
        copy = pltpu.make_async_remote_copy(
            src_ref=src, dst_ref=dst, send_sem=send_sem, recv_sem=recv_sem,
            device_id=device_id, device_id_type=MESH,
        )
        copy.start()
        started.append(copy)
        return copy

    order = list(range(1, depth))
    planes = [0] + order
    short = jnp.where(2 * z < depth, z, depth - 1 - z)
    long_side = jnp.where(2 * z < depth, 1, -1)
    inner = (z > 0) & (z < depth - 1)
    plane = {0: z}
    near = {}
    for j in order:
        both = j <= 2 * short
        gap = jnp.where(both, (j + 1) // 2, j - short)
        side = jnp.where(both & (j % 2 == 0), -long_side, long_side)
        plane[j] = z + side * gap
        near[j] = gap == 1

    owners = {}
    for j in planes:
        base = plane[j] * 4
        owners[j, 0] = base + y * 2 + x
        owners[j, 1] = base + y * 2 + (1 - x)
        owners[j, 2] = base + (1 - y) * 2 + x
        owners[j, 3] = base + (1 - y) * 2 + (1 - x)

    def views(d, place, h):
        return (
            lat_ref.at[plane[d], place, pl.ds(h * BLOCK // 2, BLOCK // 2)],
            rope_ref.at[plane[d], place, pl.ds(h * BLOCK // 4, BLOCK // 4)],
        )

    arrivals = {}
    issued = {(0, 0)}

    guarded = []

    def halved(src, dst, there, sends, recvs):
        return [
            pltpu.make_async_remote_copy(
                src_ref=a, dst_ref=b, send_sem=sends.at[part], recv_sem=recvs.at[part],
                device_id={"pool": there}, device_id_type=MESH,
            )
            for part, (a, b) in enumerate(zip(src, dst))
        ]

    def launch(condition, copies):
        if condition is None:
            for copy in copies:
                copy.start()
            started.extend(copies)
            return

        @pl.when(condition)
        def _():
            for copy in copies:
                copy.start()
        guarded.append((condition, copies))

    def pass_on(src, dst, h, sends, recvs, d, slot, there, condition=None):
        copies = halved(views(*src, h), views(*dst, h), there,
                        sends.at[plane[d], slot], recvs.at[plane[d], slot])
        launch(condition, copies)
        arrivals[dst + (h,)] = copies
        issued.add(dst)

    def take(key):
        for copy in arrivals.pop(key, ()):
            copy.wait_recv()

    def spread(d, h):
        pass_on((d, 0), (d, 1), h, x_send, x_recv, d, h, x_peer)
        pass_on((d, 0), (d, 2), 1 - h, y_send, y_recv, d, 1 - h, y_peer)

    def forward(d):
        for place, h, there, sends, recvs in (
            (1, 0, y_peer, y_send, y_recv), (2, 1, x_peer, x_send, x_recv)
        ):
            take((d, place, h))
            pass_on((d, place), (d, 3), h, sends, recvs, d, 2, there,
                    None if d == 0 else jnp.logical_not(near[d]))

    hops = ((z + 1, z < depth - 1), (z - 1, z > 0))

    def cross():
        take((0, 3, 0))
        take((0, 3, 1))
        for i, (to, exists) in enumerate(hops):
            copies = []
            for h, recvs in ((0, y_recv), (1, x_recv)):
                copies += halved(views(0, 3, h), views(0, 3, h), to * 4 + y * 2 + x,
                                 c_send.at[i, h], recvs.at[z, 2])
            launch(exists, copies)

    raw_column = {
        d: send(raw_ref, raws_ref.at[me], rz_send.at[d], rz_recv.at[d], {"pool": column[d]})
        for d in order
    }
    for h in range(2):
        spread(0, h)
    for i, (to, exists) in enumerate(hops):
        copies = []
        for h in range(2):
            copies += halved(views(0, 0, h), views(0, 0, h), to * 4 + y * 2 + x,
                             z_send.at[i, z, h], z_recv.at[z, h])
        launch(exists, copies)

    raw_copies = []

    def pass_raw(d):
        owner = column[(depth - d) % depth]
        src = raw_ref if d == 0 else raws_ref.at[owner]
        for i, there in enumerate((x_peer, y_peer, far_peer)):
            raw_copies.append(send(
                src, raws_ref.at[owner], r_send.at[d, i], r_recv.at[d, i], {"pool": there}))

    pass_raw(0)
    fetches[4].wait()
    w_copies = [
        send(w_ref, wg_ref.at[core], w_send.at[d], w_recv.at[d], {"serve": (core + d) % serve_n})
        for d in range(1, serve_n)
    ]

    def advance(d, condition):
        up = plane[d] < z
        to = jnp.where(up, z + 1, z - 1)
        further = jnp.where(up, z + 1 < depth, z > 0)
        relays = [
            halved(views(d, 0, h), views(d, 0, h), to * 4 + y * 2 + x,
                   z_send.at[jnp.where(up, 0, 1), plane[d], h], z_recv.at[plane[d], h])
            for h in range(2)
        ]
        spreads = []
        for h in range(2):
            for place, half, there, sends, recvs in (
                (1, h, x_peer, x_send, x_recv), (2, 1 - h, y_peer, y_send, y_recv)
            ):
                copies = halved(views(d, 0, half), views(d, place, half), there,
                                sends.at[plane[d], half], recvs.at[plane[d], half])
                arrivals[d, place, half] = copies
                spreads.append(copies)

        @pl.when(condition)
        def _():
            for h in range(2):
                for copy in relays[h]:
                    copy.wait_recv()

                @pl.when(further)
                def _():
                    for copy in relays[h]:
                        copy.start()
            for copies in spreads:
                for copy in copies:
                    copy.start()
        guarded.append((condition, sum(spreads, [])))
        guarded.append((condition & further, sum(relays, [])))

    def both_done(d):
        issued.update(((d, 0), (d, 1), (d, 2)))

    for fetch in fetches[6:]:
        fetch.wait()
    index = lax.broadcasted_iota(jnp.int32, (1, PPAGES), 1)
    held = jnp.clip(len_ref[0] - PAGE * index, 0, PAGE).astype(jnp.float32)
    named = named_ref[...] == lax.broadcasted_iota(jnp.int32, (n, PPAGES), 0)
    before = (
        lax.broadcasted_iota(jnp.int32, (PPAGES, PPAGES), 0)
        < lax.broadcasted_iota(jnp.int32, (PPAGES, PPAGES), 1)
    )
    rank = jnp.dot(
        jnp.where(named, 1.0, 0.0).astype(jnp.bfloat16),
        jnp.where(before, 1.0, 0.0).astype(jnp.bfloat16),
        preferred_element_type=jnp.float32,
    )
    for r in range(HOT):
        count = jnp.sum(
            jnp.where(named & (rank == r), jnp.broadcast_to(held, (n, PPAGES)), 0.0),
            axis=1, keepdims=True,
        )
        count_ref[r] = jnp.broadcast_to(count, (n, LANES))

    raws_ref[pl.ds(me, 1)] = raw_ref[...][None]
    wg_ref[pl.ds(core, 1)] = w_ref[...][None]
    fetches[5].wait()
    unit = jnp.where(
        lax.broadcasted_iota(jnp.int32, (SUF, WIDE - LAT), 1) == 0, 1.0, 0.0
    ).astype(jnp.bfloat16)
    for h in range(heads):
        qs_ref[h * SUF:(h + 1) * SUF, :] = jnp.concatenate(
            [q_ref[:, h * LAT:(h + 1) * LAT], unit], axis=1
        )

    def unpack(place, d, at):
        for r in range(HOT):
            rope = rope_ref[plane[d], place, r * PAIR:(r + 1) * PAIR, :].astype(jnp.float32)
            count = count_ref[r, pl.ds(owners[d, place], 1), :]
            turned = pltpu.roll(rope, ROPE, 1)
            line = lax.broadcasted_iota(jnp.int32, (PAIR, LANES), 0).astype(jnp.float32)
            for k, values in enumerate((rope, turned)):
                absent = (lane == ROPE) & (2.0 * line + k >= count)
                tile = jnp.where(lane < ROPE, values, jnp.where(absent, masked_score, 0.0))
                kr_ref[at + r * PAGE + k * PAIR:at + r * PAGE + (k + 1) * PAIR, :] = tile.astype(
                    jnp.bfloat16)

    for d in order:
        raw_column[d].wait_recv()
        pass_raw(d)

    blocks = [(0, 0), (0, 1), (0, 2), (0, 3)]
    for d in order[:-1]:
        blocks += [(d, 0), (d, 1), (d, 2)]
    blocks += [(order[-1], 0)] + [(d, 3) for d in order[:-1]]
    blocks += [(order[-1], 1), (order[-1], 2), (order[-1], 3)]
    pages = [(i, d, place, r) for i, (d, place) in enumerate(blocks) for r in range(HOT)]
    cuts = sorted({len(pages)} | set(range(8, len(pages), 12)) | set(range(12, len(pages), 12)))
    chunks = [pages[a:b] for a, b in zip([0] + cuts[:-1], cuts)]

    tiles = heads * SUF // TILE

    def loader(chunk):
        def latents(first, count):
            return jnp.concatenate(
                [lat_ref[plane[d], place, r * PAGE:(r + 1) * PAGE, :]
                 for _, d, place, r in chunk[first // PAGE:(first + count) // PAGE]], axis=0)

        def keys(first, count):
            at = (chunk[0][0] * HOT + chunk[0][3]) * PAGE + first
            return jnp.concatenate([latents(first, count), kr_ref[at:at + count, :]], axis=1)

        return latents, keys, len(chunk) * PAGE

    def suffix_loader():
        return (
            lambda first, count: sfx_ref[first:first + count, :VLAT],
            lambda first, count: sfx_ref[first:first + count, :],
            SUF,
        )

    def score(t, load, slot):
        _, keys, size = load
        for at in range(0, size, SUB):
            width = min(SUB, size - at)
            s_ref[slot, :, at:at + width] = lax.dot_general(
                qs_ref[t * TILE:(t + 1) * TILE, :], keys(at, width), contract_last,
                preferred_element_type=jnp.float32,
            )

    def absorb(t, load, slot, first, causal):
        latents, _, size = load
        rows = slice(t * TILE, (t + 1) * TILE)
        strips = [s_ref[slot, :, c * LANES:(c + 1) * LANES] for c in range(size // LANES)]
        if causal:
            row = lax.broadcasted_iota(jnp.int32, (TILE, LANES), 0) % SUF
            col = lax.broadcasted_iota(jnp.int32, (TILE, LANES), 1)
            for c in range(size // LANES):
                token = c * LANES + col
                token = jnp.where(token < SUF // 2, 2 * token, 2 * token - SUF + 1)
                strips[c] = jnp.where(token <= row, strips[c], masked_score)
        top = strips[0]
        for strip in strips[1:]:
            top = jnp.maximum(top, strip)
        top = jnp.broadcast_to(jnp.max(top, axis=1, keepdims=True), (TILE, LANES))
        if not first:
            earlier = top_ref[rows, :]
            top = jnp.maximum(top, earlier)
        shift = top * exp2_scale
        weights = []
        added = None
        for strip in strips:
            weight = jnp.exp2(strip * exp2_scale - shift)
            added = weight if added is None else added + weight
            weights.append(weight.astype(jnp.bfloat16))
        mixed = jnp.dot(
            jnp.concatenate(weights, axis=1), latents(0, size), preferred_element_type=jnp.float32
        )
        if not first:
            rescale = jnp.exp2((earlier - top) * exp2_scale)
            added = added + sum_ref[rows, :] * rescale
            mixed = mixed + acc_ref[rows, :] * jnp.concatenate([rescale] * (VLAT // LANES), axis=1)
        top_ref[rows, :] = top
        sum_ref[rows, :] = added
        acc_ref[rows, :] = mixed

    def advance_inner(d):
        advance(d, inner)

    def advance_outer(d):
        advance(d, jnp.logical_not(inner))
        both_done(d)

    def step(action, *places):
        return [functools.partial(action, d) for d in places]

    pending = step(forward, 0) + step(advance_inner, 1, 2) + step(advance_outer, 1) + [cross]
    pending += step(advance_inner, *order[2:]) + step(advance_outer, 2) + step(forward, 1, 2)
    for d in order[2:]:
        pending += step(advance_outer, d) + step(forward, d)

    def communicate(steps):
        for _ in range(min(steps, len(pending))):
            pending.pop(0)()

    def prepare_suffix():
        for copy in raw_copies:
            copy.wait_recv()
        for o in range(n):
            rawf_ref[o * raw_rows:(o + 1) * raw_rows, :] = raws_ref[o].astype(jnp.float32)
        wide_lane = lax.broadcasted_iota(jnp.int32, (SUF // 2, LANES), 1)
        parts, odd, last = halves(rawf_ref, 0, SUF // 2, wide_lane)
        for c in range(4):
            at = slice(c * LANES, (c + 1) * LANES)
            sfx_ref[:SUF // 2, at] = parts[c].astype(jnp.bfloat16)
            sfx_ref[SUF // 2:, at] = odd[c].astype(jnp.bfloat16)
        for half, values in enumerate((parts[4], last)):
            sfx_ref[half * SUF // 2:(half + 1) * SUF // 2, VLAT:] = jnp.where(
                wide_lane < ROPE, values, 0.0).astype(jnp.bfloat16)

    def write_page():
        page = jnp.int32(0)
        slot = jnp.int32(-1)
        for m in range(NEWP):
            mine = new_owner_ref[0, m] == me
            page = jnp.where(mine, m, page)
            slot = jnp.where(mine, new_slot_ref[0, m], slot)
        chosen = lax.broadcasted_iota(jnp.int32, (SLOTS, LANES), 0) == slot

        def write(u, carry):
            for k in range(PAIR_ROWS):
                at = pl.multiple_of(u * PAIR_ROWS * LANES, LANES) + k * LANES
                fresh = rawf_ref[pl.ds(page * FLAT + u * PAIR_ROWS + k, 1), :]
                to = pl.multiple_of(u * PAIR_ROWS * SHELF, SHELF) + k * SHELF
                kept = poolf_ref[pl.ds(to, SLOTS), :]
                new_ref[:, pl.ds(at, LANES)] = jnp.where(chosen, fresh, kept).astype(jnp.bfloat16)
            return carry

        lax.fori_loop(0, PAIR, write, 0)

    steps = [{1: 1, 3: 1}, {1: 1}, {1: 1}, {2: 2}, {}, {2: 1}]

    def finish(t):
        for h in range(t * TILE // SUF, (t + 1) * TILE // SUF):
            rows = slice(h * SUF, (h + 1) * SUF)
            share = 1.0 / jnp.sum(sum_ref[rows, :], axis=1, keepdims=True)
            mixed = (acc_ref[rows, :] * share).astype(jnp.bfloat16)
            out_ref[:, h * VHEAD:(h + 1) * VHEAD] = jnp.dot(
                mixed, wg_ref[:, h].reshape(VLAT, VHEAD), preferred_element_type=jnp.float32
            ).astype(jnp.bfloat16)

    sequence = [0, -1] + list(range(1, len(chunks)))
    ready = 0

    def prepare(i):
        nonlocal ready
        if sequence[i] < 0:
            prepare_suffix()
            return
        while ready <= chunks[sequence[i]][-1][0]:
            d, place = blocks[ready]
            while (d, place) not in issued:
                communicate(1)
            take((d, place, 0))
            take((d, place, 1))
            unpack(place, d, ready * BLOCK)
            ready += 1
        if i + 1 == len(sequence):
            for copy in w_copies:
                copy.wait_recv()

    loads = [suffix_loader() if k < 0 else loader(chunks[k]) for k in sequence]
    communicate(4)
    prepare(0)
    score(0, loads[0], 0)
    for i, load in enumerate(loads):
        when = steps[i] if i < len(steps) else {}
        for t in range(tiles):
            if t + 1 < tiles:
                score(t + 1, load, (t + 1) % 2)
            elif i + 1 < len(loads):
                prepare(i + 1)
                score(0, loads[i + 1], 0)
            absorb(t, load, t % 2, i == 0, sequence[i] < 0)
            if i + 1 == len(loads):
                finish(t)
            communicate(when.get(t, 0))
        if i == 2:
            write_page()
    for copy in started:
        copy.wait_send()
    for condition, copies in guarded:
        @pl.when(condition)
        def _(copies=copies):
            for copy in copies:
                copy.wait_send()


def fused(n, serve_n, tables, length, *arrays):
    fresh, pages, queries, w = arrays
    depth = n // 4
    heads = queries.shape[1] // LAT
    raw = (fresh.shape[1] // LANES, LANES)
    dma = pltpu.SemaphoreType.DMA
    vmem = pl.BlockSpec(memory_space=pltpu.VMEM)
    hbm = pl.BlockSpec(memory_space=pltpu.HBM)
    bf16, f32, i32 = jnp.bfloat16, jnp.float32, jnp.int32
    rows = heads * SUF
    return pl.pallas_call(
        functools.partial(fused_kernel, n, serve_n),
        out_shape=(
            jax.ShapeDtypeStruct((SUF, heads * VHEAD), bf16),
            jax.ShapeDtypeStruct(pages.shape, bf16),
        ),
        in_specs=[hbm] * len(tables) + [pl.BlockSpec(memory_space=pltpu.SMEM)] + [hbm] * 4,
        out_specs=(vmem, vmem),
        scratch_shapes=[pltpu.SMEM(table.shape, i32) for table in tables] + [
            pltpu.VMEM(tables[0].shape, i32),
            pltpu.VMEM(fresh.shape, bf16),
            pltpu.VMEM(pages.shape, bf16),
            pltpu.VMEM((FLAT * SHELF, LANES), f32),
            pltpu.VMEM((HOT * FLAT, LANES), f32),
            pltpu.VMEM(raw, f32),
            pltpu.VMEM(raw, bf16),
            pltpu.VMEM(queries.shape, bf16),
            pltpu.VMEM(w.shape, bf16),
            pltpu.VMEM((serve_n,) + w.shape, bf16),
            pltpu.VMEM((rows, WIDE), bf16),
            pltpu.VMEM((depth, 4, BLOCK, VLAT), bf16),
            pltpu.VMEM((depth, 4, BLOCK // 2, LANES), bf16),
            pltpu.VMEM((n * BLOCK, LANES), bf16),
            pltpu.VMEM((n,) + raw, bf16),
            pltpu.VMEM((n * raw[0], LANES), f32),
            pltpu.VMEM((SUF, WIDE), bf16),
            pltpu.VMEM((HOT, n, LANES), f32),
            pltpu.VMEM((2, TILE, 12 * PAGE), f32),
            pltpu.VMEM((rows, VLAT), f32),
            pltpu.VMEM((rows, LANES), f32),
            pltpu.VMEM((rows, LANES), f32),
            dma((9,)),
            dma((2, depth, 2, 2)), dma((depth, 2, 2)),
            dma((depth, 3, 2)), dma((depth, 3, 2)),
            dma((depth, 3, 2)), dma((depth, 3, 2)),
            dma((2, 2, 2)),
            dma((serve_n,)), dma((serve_n,)),
            dma((depth,)), dma((depth,)),
            dma((depth, 3)), dma((depth, 3)),
        ],
        compiler_params=pltpu.CompilerParams(
            collective_id=0, has_side_effects=True, vmem_limit_bytes=36 * 1024 * 1024
        ),
        name="fused",
    )(*(pltpu.with_memory_space_constraint(t, pltpu.HBM) for t in tables), length,
      *(pltpu.with_memory_space_constraint(t, pltpu.HBM) for t in arrays))


def local(n, serve_n, queries, new_latent, pool, page_owner, page_slot, new_owner, new_slot,
          prefix_len, w_uv):
    tables = (page_owner, page_slot, new_owner, new_slot)
    attended, updated = fused(n, serve_n, tables, prefix_len, new_latent, pool[0], queries[0], w_uv)
    return (attended[None], updated[None])


def solution(mesh):
    in_specs = (
        P("serve", None, "pool"),
        P("serve", "pool"),
        P("serve", "pool", None),
        P("serve", None),
        P("serve", None),
        P("serve", None),
        P("serve", None),
        P("serve"),
        P("pool", "serve", None),
    )
    out_specs = (P("serve", None, "pool"), P("serve", "pool", None))
    body = functools.partial(local, mesh.shape["pool"], mesh.shape["serve"])
    return jax.shard_map(body, mesh=mesh, in_specs=in_specs, out_specs=out_specs, check_vma=False)
```
